8 devices in a mesh: dp: 2 (over y, z), sp: 4 (over x, core).
Axes of the slice: x: 2, y: 2, z: 1, core: 2. Of those that a mesh axis runs over, the one named last changes fastest.
Arguments:
- q: bfloat16 [64, 32, 256], P('dp'), parts along dimension 0
- k: bfloat16 [64, 8192, 1, 256], P('dp', 'sp'), parts along dimension 0
- v: bfloat16 [64, 8192, 1, 256], P('dp', 'sp'), parts along dimension 0
Outputs:
- q: bfloat16 [64, 32, 256], P('dp'), parts along dimension 0
There are 2 independent parts. The reference program is written for one: setup_inputs(seed, part) draws one part's arguments, and reference() takes and returns one part's arrays. A program takes and returns all parts, laid end to end along the dimension named above; each array names one.
All inputs are finite; a program needn't handle non-finite values.
Results may differ from the reference program's by a relative error of at most 0.012.
Values are sent between devices in bfloat16 or wider.
A program may use at most 2 GiB of HBM per device.

```python
import jax
import jax.numpy as jnp

BATCH = 32
CACHE = 8192
HEADS = 32
KV_HEADS = 1
HEAD = 256


def setup_inputs(seed: int = 0, part: int = 0) -> dict:
    kq, kk, kv = (jax.random.fold_in(k, part) for k in jax.random.split(jax.random.key(seed), 3))
    return {
        "q": (3 * jax.random.normal(kq, (BATCH, HEADS, HEAD), jnp.float32)).astype(jnp.bfloat16),
        "k": jax.random.normal(kk, (BATCH, CACHE, KV_HEADS, HEAD), jnp.float32).astype(jnp.bfloat16),
        "v": jax.random.normal(kv, (BATCH, CACHE, KV_HEADS, HEAD), jnp.float32).astype(jnp.bfloat16),
    }


def einsum(form, a, b):
    return jnp.einsum(form, a.astype(jnp.float32), b.astype(jnp.float32))


def reference(q, k, v):
    grouped = q.reshape(BATCH, KV_HEADS, -1, HEAD)
    scores = einsum("bgsd,bugd->bgsu", grouped, k) * HEAD**-0.5
    weights = jax.nn.softmax(scores, -1).astype(jnp.bfloat16)
    return einsum("bgsu,bugd->bgsd", weights, v).astype(jnp.bfloat16).reshape(BATCH, HEADS, HEAD)
```

```python
import jax
import jax.numpy as jnp
from jax import lax
from jax.experimental import pallas as pl
from jax.experimental.pallas import tpu as pltpu
from jax.sharding import PartitionSpec as P

MESH = pl.DeviceIdType.MESH
GROUP = 4
SLOTS = 16
LEAD = 2
LOG2E = 1.4426950408889634
EXPLICIT = False


def kernel(mesh, q_hbm, k_hbm, v_hbm, o_ref, *scratch):
    def body(*accs):
        attend(q_hbm, k_hbm, v_hbm, o_ref, accs, *scratch)

    if not EXPLICIT:
        return body()
    with jax.sharding.use_abstract_mesh(mesh.abstract_mesh):
        acc = [pltpu.ACC(m)((32, 256), jnp.float32) for m in (0, 1)]
        pl.run_scoped(body, *[acc[0]] * 6, *[acc[1]] * 6)


def attend(q_hbm, k_hbm, v_hbm, o_ref, accs, q_ref, kbuf, vbuf, scores, weights, mine, theirs, part, pair, from_chip, from_core,
           q_sem, k_sem, v_sem, mine_sem, theirs_sem, part_sem, chip_sem, pair_sem, core_sem):
    count, heads, head = q_hbm.shape
    tokens = k_hbm.shape[1]
    tiles = tokens // 256
    groups = count // GROUP
    factor = head**-0.5 * LOG2E

    dp, sp = lax.axis_index("dp"), lax.axis_index("sp")
    core = sp + 1 - 2 * lax.rem(sp, 2)
    chip = lax.rem(sp + 2, 4)
    across = lax.rem(core + 2, 4)
    peers = (core, chip, across)

    def keys(s):
        return pltpu.make_async_copy(k_hbm.at[s], kbuf.at[s % SLOTS], k_sem.at[s % SLOTS])

    def values(s):
        return pltpu.make_async_copy(v_hbm.at[s], vbuf.at[s % SLOTS], v_sem.at[s % SLOTS])

    def remote(src, dst, send, recv, peer):
        return pltpu.make_async_remote_copy(src, dst, send, recv, device_id=(dp, peer), device_id_type=MESH)

    def stats(g, n):
        return remote(mine.at[g], theirs.at[g, n], mine_sem.at[g, n], theirs_sem.at[g, n], peers[n])

    def to_chip(lo, n):
        return remote(part.at[pl.ds(lo, n)], from_chip.at[pl.ds(lo, n)], part_sem.at[lo], chip_sem.at[lo], chip)

    def to_core(lo, n):
        return remote(pair.at[pl.ds(lo, n)], from_core.at[pl.ds(lo, n)], pair_sem.at[lo], core_sem.at[lo], core)

    def score(s, j):
        q, k = q_ref[s], kbuf.at[s % SLOTS]
        if not EXPLICIT:
            scores[j] = lax.dot_general(q, k[...], (((1,), (1,)), ((), ())), preferred_element_type=jnp.float32)
            return
        for t in range(tiles):
            m, u = t % 2, t // 2
            pltpu.matmul_push_rhs(k[t * 256 : (t + 1) * 256, :], u % 2, m, transpose=True)
            pltpu.matmul_acc_lhs(accs[6 * m + u], q, load_staged_rhs=u % 2)
        for t in range(tiles):
            scores[j, :, t * 256 : (t + 1) * 256] = pltpu.matmul_pop(accs[6 * (t % 2) + t // 2])

    def softmax(s, j):
        x = scores[j]
        high = jnp.max(x, 1, keepdims=True)
        w = jnp.exp2((x - high) * factor)
        weights[s % (LEAD * GROUP)] = w.astype(jnp.bfloat16)
        return high, jnp.sum(w, 1, keepdims=True)

    def gather(s, j):
        w, v = weights.at[s % (LEAD * GROUP)], vbuf.at[s % SLOTS]
        if not EXPLICIT:
            return jnp.dot(w[...], v[...], preferred_element_type=jnp.float32)
        for t in range(tiles):
            m, u = t % 2, t // 2
            pltpu.matmul_push_rhs(v[t * 256 : (t + 1) * 256, :], u % 2, m)
            pltpu.matmul_acc_lhs(accs[6 * m + 4 + j % 2], w[:, t * 256 : (t + 1) * 256], load_staged_rhs=u % 2)
        return pltpu.matmul_pop(accs[4 + j % 2]) + pltpu.matmul_pop(accs[10 + j % 2])

    def keep_stats(g, pairs):
        lane = lax.broadcasted_iota(jnp.int32, (heads, 128), 1)
        x = jnp.zeros((heads, 128), jnp.float32)
        for j, (high, total) in enumerate(pairs):
            x = jnp.where(lane == j, high, x)
            x = jnp.where(lane == GROUP + j, total, x)
        mine[g, :, :heads] = x.T[: 2 * GROUP, :]

    def shares(g):
        rows = [mine[g]] + [theirs[g, n] for n in range(3)]
        highs, totals = [r[:GROUP] for r in rows], [r[GROUP:] for r in rows]
        top = jnp.maximum(jnp.maximum(highs[0], highs[1]), jnp.maximum(highs[2], highs[3]))
        scale = [jnp.exp2((h - top) * factor) for h in highs]
        parts = [t * s for t, s in zip(totals, scale)]
        whole = (parts[0] + parts[1]) + (parts[2] + parts[3])
        share = scale[0] / whole
        return jnp.concatenate([share, jnp.zeros_like(share)], 0).T

    def add_chip(lo, n):
        a = part[lo : lo + n].astype(jnp.float32) + from_chip[lo : lo + n].astype(jnp.float32)
        pair[lo : lo + n] = a.astype(jnp.bfloat16)

    def add_core(lo, n):
        a = pair[lo : lo + n].astype(jnp.float32) + from_core[lo : lo + n].astype(jnp.float32)
        o_ref[lo : lo + n] = a.astype(jnp.bfloat16)

    pltpu.make_async_copy(q_hbm, q_ref, q_sem.at[0]).start()
    for s in range(LEAD * GROUP):
        keys(s).start()
    for s in range(SLOTS - LEAD * GROUP):
        keys(s + LEAD * GROUP).start()
        values(s).start()
    barrier = pltpu.get_barrier_semaphore()
    for peer in peers:
        pl.semaphore_signal(barrier, inc=1, device_id=(dp, peer), device_id_type=MESH)
    pltpu.make_async_copy(q_hbm, q_ref, q_sem.at[0]).wait()

    for h in range(groups + LEAD):
        g = h - LEAD
        with_keys, with_values = h < groups, g >= 0
        if with_keys and with_values and h < groups - 1:
            for j in range(GROUP):
                keys(GROUP * h + j).wait()
                values(GROUP * g + j).wait()
        if with_values:
            for n in range(3):
                stats(g, n).wait_recv()
            share = shares(g)
            if g >= 2:
                to_chip(GROUP * (g - 2), GROUP).wait_recv()
                add_chip(GROUP * (g - 2), GROUP)
            if g >= 3:
                to_core(GROUP * (g - 3), GROUP).wait_recv()
                add_core(GROUP * (g - 3), GROUP)
        pairs = []
        for j in range(GROUP):
            sk, sv = GROUP * h + j, GROUP * g + j
            alone = not (with_keys and with_values) or h == groups - 1
            if with_keys:
                if alone:
                    keys(sk).wait()
                score(sk, j)
            if with_values:
                if alone:
                    values(sv).wait()
                seen = gather(sv, j)
                part[sv] = (seen * share[:heads, j : j + 1]).astype(jnp.bfloat16)
            if with_keys:
                pairs.append(softmax(sk, j))
        if with_keys:
            keep_stats(h, pairs)
            if h == 0:
                pl.semaphore_wait(barrier, 3)
            for n in range(3):
                stats(h, n).start()
        if with_values:
            to_chip(GROUP * g, GROUP).start()
            if g >= 2:
                to_core(GROUP * (g - 2), GROUP).start()
        for j in range(GROUP):
            if GROUP * h + SLOTS + j < count:
                keys(GROUP * h + SLOTS + j).start()
            if GROUP * (g + 4) + j < count and GROUP * (g + 4) + j >= SLOTS - LEAD * GROUP:
                values(GROUP * (g + 4) + j).start()

    for g in range(groups - 2, groups):
        to_chip(GROUP * g, GROUP).wait_recv()
        add_chip(GROUP * g, GROUP)
        to_core(GROUP * g, GROUP).start()
    for g in range(groups - 3, groups):
        to_core(GROUP * g, GROUP).wait_recv()
        add_core(GROUP * g, GROUP)
    for g in range(groups):
        for n in range(3):
            stats(g, n).wait_send()
        to_chip(GROUP * g, GROUP).wait_send()
        to_core(GROUP * g, GROUP).wait_send()


def solution(mesh):
    def step(q, k, v):
        count, heads, head = q.shape
        tokens = k.shape[1]
        groups = count // GROUP
        whole = (count, heads, head)
        dma = pltpu.SemaphoreType.DMA
        return pl.pallas_call(
            lambda *refs: kernel(mesh, *refs),
            out_shape=jax.ShapeDtypeStruct(whole, jnp.bfloat16),
            in_specs=[pl.BlockSpec(memory_space=pl.ANY)] * 3,
            out_specs=pl.BlockSpec(memory_space=pltpu.VMEM),
            scratch_shapes=[
                pltpu.VMEM(whole, jnp.bfloat16),
                pltpu.VMEM((SLOTS, tokens, head), jnp.bfloat16),
                pltpu.VMEM((SLOTS, tokens, head), jnp.bfloat16),
                pltpu.VMEM((GROUP, heads, tokens), jnp.float32),
                pltpu.VMEM((LEAD * GROUP, heads, tokens), jnp.bfloat16),
                pltpu.VMEM((groups, 2 * GROUP, 128), jnp.float32),
                pltpu.VMEM((groups, 3, 2 * GROUP, 128), jnp.float32),
                *[pltpu.VMEM(whole, jnp.bfloat16)] * 4,
                dma((1,)),
                dma((SLOTS,)),
                dma((SLOTS,)),
                dma((groups, 3)),
                dma((groups, 3)),
                *[dma((count,))] * 4,
            ],
            compiler_params=pltpu.CompilerParams(collective_id=0, has_side_effects=True, vmem_limit_bytes=60 * 2**20),
            name="attend",
        )(q, k.reshape(count, tokens, head), v.reshape(count, tokens, head))

    return jax.shard_map(
        step,
        mesh=mesh,
        in_specs=(P("dp", None, None), P("dp", "sp", None, None), P("dp", "sp", None, None)),
        out_specs=P("dp", None, None),
        check_vma=False,
    )
```

```python
import jax
import jax.numpy as jnp
from jax import lax
from jax.experimental import pallas as pl
from jax.experimental.pallas import tpu as pltpu
from jax.sharding import PartitionSpec as P

MESH = pl.DeviceIdType.MESH
GROUP = 4
SLOTS = 16
LEAD = 2
LOG2E = 1.4426950408889634
WEIGHTS = (LEAD + 1) * GROUP
COMM = {
    4: ((0, "core", 0),),
    5: ((1, "core", 0),),
    6: ((2, "core", 0),),
    7: ((3, "core", 0), (0, "chip", 0)),
    ("v", 21): ((4, "core", 0), (1, "chip", 0)),
    ("v", 23): ((2, "chip", 0),),
    ("v", 25): ((3, "chip", 0),),
    ("v", 26): ((5, "core", 0),),
    ("v", 28): ((4, "chip", 0),),
    ("v", 29): ((6, "core", 0),),
    "end": ((5, "chip", 0),),
    "end2": ((6, "chip", 0),),
}


def attend(q_hbm, k_hbm, v_hbm, o_ref, q_ref, kbuf, vbuf, scores, weights, mine, theirs, own, part, from_core, pair, from_chip, pair_last, chip_last, core_last,
           q_sem, k_sem, v_sem, mine_sem, theirs_sem, part_sem, core_sem, pair_sem, chip_sem, done_sem, out_sem, last_sem):
    count, heads, head = q_hbm.shape
    tokens = k_hbm.shape[1]
    groups = count // GROUP
    half = heads // 2
    last = count - GROUP
    factor = head**-0.5 * LOG2E

    dp, sp = lax.axis_index("dp"), lax.axis_index("sp")
    side = lax.rem(sp, 2)
    core = sp + 1 - 2 * side
    chip = lax.rem(sp + 2, 4)
    peers = (core, chip, lax.rem(core + 2, 4))
    rows = pl.ds(pl.multiple_of(side * half, half), half)
    other_rows = pl.ds(pl.multiple_of((1 - side) * half, half), half)

    def keys(s):
        return pltpu.make_async_copy(k_hbm.at[s], kbuf.at[s % SLOTS], k_sem.at[s % SLOTS])

    def values(s):
        return pltpu.make_async_copy(v_hbm.at[s], vbuf.at[s % SLOTS], v_sem.at[s % SLOTS])

    def remote(src, dst, send, recv, peer):
        return pltpu.make_async_remote_copy(src, dst, send, recv, device_id=(dp, peer), device_id_type=MESH)

    def stats(g, n):
        return remote(mine.at[g], theirs.at[g, n], mine_sem.at[g, n], theirs_sem.at[g, n], peers[n])

    def span(g):
        return pl.ds(GROUP * g, GROUP)

    def halves(g):
        return remote(part.at[span(g), other_rows], from_core.at[span(g)], part_sem.at[g], core_sem.at[g], core)

    def sums(g):
        return remote(pair.at[span(g)], from_chip.at[span(g)], pair_sem.at[g], chip_sem.at[g], chip)

    def results(g):
        return remote(o_ref.at[span(g), rows], o_ref.at[span(g), rows], done_sem.at[g], out_sem.at[g], core)

    def last_chip(j):
        return remote(part.at[last + j], chip_last.at[j], last_sem.at[0, j], last_sem.at[1, j], chip)

    def last_core(j):
        return remote(pair_last.at[j], core_last.at[j], last_sem.at[2, j], last_sem.at[3, j], core)

    def score(s):
        scores[s % GROUP] = lax.dot_general(
            q_ref[s], kbuf[s % SLOTS], (((1,), (1,)), ((), ())), preferred_element_type=jnp.float32
        )

    def softmax(s):
        x = scores[s % GROUP]
        high = jnp.max(x, 1, keepdims=True)
        w = jnp.exp2((x - high) * factor)
        weights[s % WEIGHTS] = w.astype(jnp.bfloat16)
        return high, jnp.sum(w, 1, keepdims=True)

    def gather(s, share):
        seen = jnp.dot(weights[s % WEIGHTS], vbuf[s % SLOTS], preferred_element_type=jnp.float32)
        seen = seen * share[:heads, s % GROUP : s % GROUP + 1]
        own[s] = seen
        part[s] = seen.astype(jnp.bfloat16)

    def keep_stats(g, pairs):
        lane = lax.broadcasted_iota(jnp.int32, (heads, 128), 1)
        x = jnp.zeros((heads, 128), jnp.float32)
        for j, (high, total) in enumerate(pairs):
            x = jnp.where(lane == j, high, x)
            x = jnp.where(lane == GROUP + j, total, x)
        mine[g, :, :heads] = x.T[: 2 * GROUP, :]

    def shares(g):
        for n in range(3):
            stats(g, n).wait_recv()
        rows = [mine[g]] + [theirs[g, n] for n in range(3)]
        highs, totals = [r[:GROUP] for r in rows], [r[GROUP:] for r in rows]
        top = jnp.maximum(jnp.maximum(highs[0], highs[1]), jnp.maximum(highs[2], highs[3]))
        scale = [jnp.exp2((h - top) * factor) for h in highs]
        parts = [t * s for t, s in zip(totals, scale)]
        whole = (parts[0] + parts[1]) + (parts[2] + parts[3])
        share = scale[0] / whole
        return jnp.concatenate([share, jnp.zeros_like(share)], 0).T

    def add_core(g):
        halves(g).wait_recv()
        pair[span(g)] = (own[span(g), rows] + from_core[span(g)].astype(jnp.float32)).astype(jnp.bfloat16)

    def add_chip(g):
        sums(g).wait_recv()
        o_ref[span(g), rows] = (pair[span(g)].astype(jnp.float32) + from_chip[span(g)].astype(jnp.float32)).astype(jnp.bfloat16)

    order = [("k", s) for s in range(LEAD * GROUP)]
    for s in range(count - (LEAD + 1) * GROUP):
        order += [("k", s + LEAD * GROUP), ("v", s)]
    order += [("k", s) for s in range(last, count)] + [("v", s) for s in range(count - (LEAD + 1) * GROUP, count)]

    def start(used_k, used_v):
        while order and order[0][1] < SLOTS + {"k": used_k, "v": used_v}[order[0][0]]:
            kind, s = order.pop(0)
            (keys if kind == "k" else values)(s).start(priority=1)

    pltpu.make_async_copy(q_hbm, q_ref, q_sem.at[0]).start()
    start(0, 0)
    barrier = pltpu.get_barrier_semaphore()
    for peer in peers:
        pl.semaphore_signal(barrier, inc=1, device_id=(dp, peer), device_id_type=MESH)
    pltpu.make_async_copy(q_hbm, q_ref, q_sem.at[0]).wait()

    for h in range(groups):
        g = h - LEAD
        paired = g >= 0 and h < groups - 1
        share = None
        if paired:
            for j in range(GROUP):
                keys(GROUP * h + j).wait()
                values(GROUP * g + j).wait()
            share = shares(g)
        sends = []
        for done, act, nxt in COMM.get(h, ()):
            (add_core if act == "core" else add_chip)(done)
            sends.append(sums(done) if act == "core" else results(done))
        pairs = []
        for j in range(GROUP):
            if not paired:
                keys(GROUP * h + j).wait()
            score(GROUP * h + j)
            if paired:
                gather(GROUP * g + j, share)
            pairs.append(softmax(GROUP * h + j))
        keep_stats(h, pairs)
        if h == 0:
            pl.semaphore_wait(barrier, 3)
        sends += [stats(h, n) for n in range(3)]
        if paired:
            sends.append(halves(g))
        for send in sends:
            send.start()
        start(GROUP * (h + 1), GROUP * (g + 1) if paired else 0 if g < 0 else GROUP * g)

    for s in range(count - (LEAD + 1) * GROUP, count):
        g, j = s // GROUP, s % GROUP
        if j == 0:
            share = shares(g)
        values(s).wait()
        gather(s, share)
        if g == groups - 1:
            last_chip(j).start()
        elif j == GROUP - 1:
            halves(g).start()
        for done, act, nxt in COMM.get(("v", s), ()):
            (add_core if act == "core" else add_chip)(done)
            (sums(done) if act == "core" else results(done)).start()

    for done, act, nxt in COMM["end"]:
        (add_core if act == "core" else add_chip)(done)
        (sums(done) if act == "core" else results(done)).start()
    for j in range(GROUP):
        last_chip(j).wait_recv()
        pair_last[j] = (part[last + j].astype(jnp.float32) + chip_last[j].astype(jnp.float32)).astype(jnp.bfloat16)
        last_core(j).start()
    for done, act, nxt in COMM["end2"]:
        (add_core if act == "core" else add_chip)(done)
        (sums(done) if act == "core" else results(done)).start()
    for j in range(GROUP):
        last_core(j).wait_recv()
        o_ref[last + j] = (pair_last[j].astype(jnp.float32) + core_last[j].astype(jnp.float32)).astype(jnp.bfloat16)
    for g in range(groups):
        for n in range(3):
            stats(g, n).wait_send()
    for g in range(groups - 1):
        halves(g).wait_send()
        sums(g).wait_send()
        results(g).wait()
    for j in range(GROUP):
        last_chip(j).wait_send()
        last_core(j).wait_send()


def solution(mesh):
    def step(q, k, v):
        count, heads, head = q.shape
        tokens = k.shape[1]
        groups = count // GROUP
        whole = (count, heads, head)
        dma = pltpu.SemaphoreType.DMA
        hbm = pl.BlockSpec(memory_space=pltpu.HBM)
        return pl.pallas_call(
            attend,
            out_shape=jax.ShapeDtypeStruct(whole, jnp.bfloat16),
            in_specs=[hbm] * 3,
            out_specs=pl.BlockSpec(memory_space=pltpu.VMEM),
            scratch_shapes=[
                pltpu.VMEM(whole, jnp.bfloat16),
                pltpu.VMEM((SLOTS, tokens, head), jnp.bfloat16),
                pltpu.VMEM((SLOTS, tokens, head), jnp.bfloat16),
                pltpu.VMEM((GROUP, heads, tokens), jnp.float32),
                pltpu.VMEM((WEIGHTS, heads, tokens), jnp.bfloat16),
                pltpu.VMEM((groups, 2 * GROUP, 128), jnp.float32),
                pltpu.VMEM((groups, 3, 2 * GROUP, 128), jnp.float32),
                pltpu.VMEM(whole, jnp.float32),
                pltpu.VMEM(whole, jnp.bfloat16),
                *[pltpu.VMEM((count, heads // 2, head), jnp.bfloat16)] * 3,
                *[pltpu.VMEM((GROUP, heads, head), jnp.bfloat16)] * 3,
                dma((1,)),
                dma((SLOTS,)),
                dma((SLOTS,)),
                dma((groups, 3)),
                dma((groups, 3)),
                *[dma((groups,))] * 6,
                dma((4, GROUP)),
            ],
            compiler_params=pltpu.CompilerParams(collective_id=0, has_side_effects=True, vmem_limit_bytes=44 * 2**20),
            name="attend",
        )(q, k.reshape(count, tokens, head), v.reshape(count, tokens, head))

    return jax.shard_map(
        step,
        mesh=mesh,
        in_specs=(P("dp", None, None), P("dp", "sp", None, None), P("dp", "sp", None, None)),
        out_specs=P("dp", None, None),
        check_vma=False,
    )
```

```python
import jax
import jax.numpy as jnp
from jax import lax
from jax.experimental import pallas as pl
from jax.experimental.pallas import tpu as pltpu
from jax.sharding import PartitionSpec as P

MESH = pl.DeviceIdType.MESH
GROUP = 4
SLOTS = 32
LOG2E = 1.4426950408889634
BLOCKS = [range(4 * g, 4 * g + 4) for g in range(6)] + [range(24, 26), range(26, 28)] + [range(s, s + 1) for s in range(28, 32)]
SUMS = {
    1: (("core", 0),),
    2: (("core", 1),),
    3: (("core", 2),),
    4: (("chip", 0), ("core", 3)),
    5: (("chip", 1), ("core", 4)),
    7: (("chip", 2),),
    8: (("core", 5),),
    9: (("chip", 3),),
    11: (("core", 6), ("chip", 4)),
    "end": (("chip", 5),),
    "end2": (("chip", 6),),
}


def attend(q_hbm, k_hbm, v_hbm, o_ref, q_ref, buf, scores, weights, mine, theirs, own, part, from_core, pair, from_chip, pair_last, chip_last, core_last,
           q_sem, buf_sem, mine_sem, theirs_sem, part_sem, core_sem, pair_sem, chip_sem, done_sem, out_sem, last_sem):
    count, heads, head = q_hbm.shape
    tokens = k_hbm.shape[1]
    groups = count // GROUP
    half = heads // 2
    last = count - GROUP
    factor = head**-0.5 * LOG2E

    dp, sp = lax.axis_index("dp"), lax.axis_index("sp")
    side = lax.rem(sp, 2)
    core = sp + 1 - 2 * side
    chip = lax.rem(sp + 2, 4)
    peers = (core, chip, lax.rem(core + 2, 4))
    rows = pl.ds(pl.multiple_of(side * half, half), half)
    other_rows = pl.ds(pl.multiple_of((1 - side) * half, half), half)

    def keys(s):
        return pltpu.make_async_copy(k_hbm.at[s], buf.at[s % SLOTS], buf_sem.at[s % SLOTS])

    def values(s):
        n = count + s
        return pltpu.make_async_copy(v_hbm.at[s], buf.at[n % SLOTS], buf_sem.at[n % SLOTS])

    def remote(src, dst, send, recv, peer):
        return pltpu.make_async_remote_copy(src, dst, send, recv, device_id=(dp, peer), device_id_type=MESH)

    def stats(g, n):
        return remote(mine.at[g], theirs.at[g, n], mine_sem.at[g, n], theirs_sem.at[g, n], peers[n])

    def span(g):
        return pl.ds(GROUP * g, GROUP)

    def halves(g):
        return remote(part.at[span(g), other_rows], from_core.at[span(g)], part_sem.at[g], core_sem.at[g], core)

    def sums(g):
        return remote(pair.at[span(g)], from_chip.at[span(g)], pair_sem.at[g], chip_sem.at[g], chip)

    def results(g):
        return remote(o_ref.at[span(g), rows], o_ref.at[span(g), rows], done_sem.at[g], out_sem.at[g], core)

    def last_chip(j):
        return remote(part.at[last + j], chip_last.at[j], last_sem.at[0, j], last_sem.at[1, j], chip)

    def last_core(j):
        return remote(pair_last.at[j], core_last.at[j], last_sem.at[2, j], last_sem.at[3, j], core)

    def score(s):
        scores[s % GROUP] = lax.dot_general(
            q_ref[s], buf[s % SLOTS], (((1,), (1,)), ((), ())), preferred_element_type=jnp.float32
        )

    def softmax(s):
        x = scores[s % GROUP]
        high = jnp.max(x, 1, keepdims=True)
        w = jnp.exp2((x - high) * factor)
        weights[s] = w.astype(jnp.bfloat16)
        return high, jnp.sum(w, 1, keepdims=True)

    def gather(s, share):
        n = (count + s) % SLOTS
        seen = [jnp.dot(weights[s], buf[n, :, c : c + 128], preferred_element_type=jnp.float32) for c in range(0, head, 128)]
        seen = jnp.concatenate(seen, 1) * share[:heads, s % GROUP : s % GROUP + 1]
        own[s] = seen
        part[s] = seen.astype(jnp.bfloat16)

    def keep_stats(g, pairs):
        lane = lax.broadcasted_iota(jnp.int32, (heads, 128), 1)
        x = jnp.zeros((heads, 128), jnp.float32)
        for j, (high, total) in enumerate(pairs):
            x = jnp.where(lane == j, high, x)
            x = jnp.where(lane == GROUP + j, total, x)
        mine[g, :, :heads] = x.T[: 2 * GROUP, :]

    def shares(g):
        for n in range(3):
            stats(g, n).wait_recv()
        rows = [mine[g]] + [theirs[g, n] for n in range(3)]
        highs, totals = [r[:GROUP] for r in rows], [r[GROUP:] for r in rows]
        top = jnp.maximum(jnp.maximum(highs[0], highs[1]), jnp.maximum(highs[2], highs[3]))
        scale = [jnp.exp2((h - top) * factor) for h in highs]
        parts = [t * s for t, s in zip(totals, scale)]
        whole = (parts[0] + parts[1]) + (parts[2] + parts[3])
        share = scale[0] / whole
        return jnp.concatenate([share, jnp.zeros_like(share)], 0).T

    def add_core(g):
        halves(g).wait_recv()
        pair[span(g)] = (own[span(g), rows] + from_core[span(g)].astype(jnp.float32)).astype(jnp.bfloat16)

    def add_chip(g):
        sums(g).wait_recv()
        o_ref[span(g), rows] = (pair[span(g)].astype(jnp.float32) + from_chip[span(g)].astype(jnp.float32)).astype(jnp.bfloat16)

    def sum_parts(step):
        for over, g in SUMS.get(step, ()):
            if over == "core":
                add_core(g)
                sums(g).start()
            else:
                add_chip(g)
                results(g).start()

    pltpu.make_async_copy(q_hbm, q_ref, q_sem.at[0]).start()
    for n in range(SLOTS):
        keys(n).start(priority=1)
    barrier = pltpu.get_barrier_semaphore()
    for peer in peers:
        pl.semaphore_signal(barrier, inc=1, device_id=(dp, peer), device_id_type=MESH)
    pltpu.make_async_copy(q_hbm, q_ref, q_sem.at[0]).wait()

    pairs = []

    def send_stats(g):
        keep_stats(g, [pairs.pop(0) for _ in range(GROUP)])
        if g == 0:
            pl.semaphore_wait(barrier, 3)
        for n in range(3):
            stats(g, n).start()

    for g in range(groups):
        for s in range(GROUP * g, GROUP * g + GROUP):
            keys(s).wait()
        for s in range(GROUP * g, GROUP * g + GROUP):
            score(s)
            if s:
                pairs.append(softmax(s - 1))
        if g:
            send_stats(g - 1)
        for s in range(GROUP * g, GROUP * g + GROUP):
            values(s).start(priority=1)
    pairs.append(softmax(count - 1))
    send_stats(groups - 1)

    for step, block in enumerate(BLOCKS):
        for s in block:
            values(s).wait()
        g = block[0] // GROUP
        if block[0] % GROUP == 0:
            share = shares(g)
        for s in block:
            gather(s, share)
        if g == groups - 1:
            last_chip(block[0] % GROUP).start()
        elif block[-1] % GROUP == GROUP - 1:
            halves(g).start()
        sum_parts(step)

    sum_parts("end")
    for j in range(GROUP):
        last_chip(j).wait_recv()
        pair_last[j] = (part[last + j].astype(jnp.float32) + chip_last[j].astype(jnp.float32)).astype(jnp.bfloat16)
        last_core(j).start()
    sum_parts("end2")
    for j in range(GROUP):
        last_core(j).wait_recv()
        o_ref[last + j] = (pair_last[j].astype(jnp.float32) + core_last[j].astype(jnp.float32)).astype(jnp.bfloat16)
    for g in range(groups):
        for n in range(3):
            stats(g, n).wait_send()
    for g in range(groups - 1):
        halves(g).wait_send()
        sums(g).wait_send()
        results(g).wait()
    for j in range(GROUP):
        last_chip(j).wait_send()
        last_core(j).wait_send()


def solution(mesh):
    def step(q, k, v):
        count, heads, head = q.shape
        tokens = k.shape[1]
        groups = count // GROUP
        whole = (count, heads, head)
        dma = pltpu.SemaphoreType.DMA
        hbm = pl.BlockSpec(memory_space=pltpu.HBM)
        return pl.pallas_call(
            attend,
            out_shape=jax.ShapeDtypeStruct(whole, jnp.bfloat16),
            in_specs=[hbm] * 3,
            out_specs=pl.BlockSpec(memory_space=pltpu.VMEM),
            scratch_shapes=[
                pltpu.VMEM(whole, jnp.bfloat16),
                pltpu.VMEM((SLOTS, tokens, head), jnp.bfloat16),
                pltpu.VMEM((GROUP, heads, tokens), jnp.float32),
                pltpu.VMEM((count, heads, tokens), jnp.bfloat16),
                pltpu.VMEM((groups, 2 * GROUP, 128), jnp.float32),
                pltpu.VMEM((groups, 3, 2 * GROUP, 128), jnp.float32),
                pltpu.VMEM(whole, jnp.float32),
                pltpu.VMEM(whole, jnp.bfloat16),
                *[pltpu.VMEM((count, heads // 2, head), jnp.bfloat16)] * 3,
                *[pltpu.VMEM((GROUP, heads, head), jnp.bfloat16)] * 3,
                dma((1,)),
                dma((SLOTS,)),
                dma((groups, 3)),
                dma((groups, 3)),
                *[dma((groups,))] * 6,
                dma((4, GROUP)),
            ],
            compiler_params=pltpu.CompilerParams(collective_id=0, has_side_effects=True, vmem_limit_bytes=48 * 2**20),
            name="attend",
        )(q, k.reshape(count, tokens, head), v.reshape(count, tokens, head))

    return jax.shard_map(
        step,
        mesh=mesh,
        in_specs=(P("dp", None, None), P("dp", "sp", None, None), P("dp", "sp", None, None)),
        out_specs=P("dp", None, None),
        check_vma=False,
    )
```

```python
import jax
import jax.numpy as jnp
from jax import lax
from jax.experimental import pallas as pl
from jax.experimental.pallas import tpu as pltpu
from jax.sharding import PartitionSpec as P

MESH = pl.DeviceIdType.MESH
LOG2E = 1.4426950408889634
SLOTS = 32
READS = 14
STATS = 8
SCORES = 4

BLOCKS = (
    [("k", s, 4) for s in (0, 4, 8, 12, 16)]
    + [("v", 0, 4), ("k", 20, 4), ("v", 4, 4), ("k", 24, 4), ("v", 8, 4), ("k", 28, 4), ("v", 12, 4), ("v", 16, 4)]
    + [("v", s, 2) for s in (20, 22, 24, 26)]
    + [("v", s, 1) for s in (28, 29, 30, 31)]
)
SPANS = [(s, n) for kind, s, n in BLOCKS if kind == "v" and s < 28]
LATE = (28, 29, 30)
FINAL = 31
SUMS = {
    6: ("core0",),
    8: ("core1",),
    9: ("chip0",),
    10: ("core2",),
    11: ("chip1",),
    12: ("core3",),
    13: ("chip2",),
    15: ("core4", "core5"),
    16: ("core6",),
    18: ("core7",),
    20: ("core8", "chip3"),
}
DRAIN = ("chip4", "chip5", "chip6", "late0", "late1", "chip7", "late2", "final", "chip8")


def attend(q_hbm, k_hbm, v_hbm, o_ref, q_ref, buf, scores, weights, mine, theirs, own, part, from_core, pair, from_chip, late_pair, late_chip, late_core, final_in,
           q_sem, buf_sem, stats_out, stats_in, core_out, core_in, chip_out, chip_in, done_out, done_in, late_out, late_chip_in, late_core_in, final_sem):
    count, heads, head = q_hbm.shape
    half = heads // 2
    factor = head**-0.5 * LOG2E

    dp, sp = lax.axis_index("dp"), lax.axis_index("sp")
    side = lax.rem(sp, 2)
    core = sp + 1 - 2 * side
    chip = lax.rem(sp + 2, 4)
    peers = (core, chip, lax.rem(core + 2, 4))
    rows = pl.ds(pl.multiple_of(side * half, half), half)
    other_rows = pl.ds(pl.multiple_of((1 - side) * half, half), half)

    first = [sum(n for _, _, n in BLOCKS[:b]) for b in range(len(BLOCKS))]
    slot_of = {(kind, s + i): (first[b] + i) % SLOTS for b, (kind, s, n) in enumerate(BLOCKS) for i in range(n)}

    def read(b):
        kind, s, n = BLOCKS[b]
        src = k_hbm if kind == "k" else v_hbm
        return pltpu.make_async_copy(src.at[pl.ds(s, n)], buf.at[pl.ds(first[b] % SLOTS, n)], buf_sem.at[b % READS])

    def remote(src, dst, send, recv, peer):
        return pltpu.make_async_remote_copy(src, dst, send, recv, device_id=(dp, peer), device_id_type=MESH)

    def stats(g, n):
        return remote(mine.at[g], theirs.at[g, n], stats_out, stats_in.at[g], peers[n])

    def span(c):
        return pl.ds(*SPANS[c])

    def halves(c):
        return remote(part.at[span(c), other_rows], from_core.at[span(c)], core_out, core_in.at[c], core)

    def sums(c):
        return remote(pair.at[span(c)], from_chip.at[span(c)], chip_out, chip_in.at[c], chip)

    def results(c):
        return remote(o_ref.at[span(c), rows], o_ref.at[span(c), rows], done_out, done_in, core)

    def to_chip(i):
        return remote(part.at[LATE[i]], late_chip.at[i], late_out, late_chip_in.at[i], chip)

    def to_core(i):
        return remote(late_pair.at[i], late_core.at[i], late_out, late_core_in.at[i], core)

    def to_all(n):
        return remote(part.at[FINAL], final_in.at[n], late_out, final_sem, peers[n])

    def add(a, b):
        return a.astype(jnp.float32) + b.astype(jnp.float32)

    def score(s):
        scores[s % SCORES] = lax.dot_general(
            q_ref[s], buf[slot_of["k", s]], (((1,), (1,)), ((), ())), preferred_element_type=jnp.float32
        )

    def softmax(s):
        x = scores[s % SCORES]
        high = jnp.max(x, 1, keepdims=True)
        w = jnp.exp2((x - high) * factor)
        weights[s] = w.astype(jnp.bfloat16)
        return high, jnp.sum(w, 1, keepdims=True)

    def gather(s, share):
        v = slot_of["v", s]
        seen = [jnp.dot(weights[s], buf[v, :, c : c + 128], preferred_element_type=jnp.float32) for c in range(0, head, 128)]
        seen = jnp.concatenate(seen, 1) * share[:heads, s % STATS : s % STATS + 1]
        own[s] = seen
        part[s] = seen.astype(jnp.bfloat16)

    def send_stats(g, pairs):
        lane = lax.broadcasted_iota(jnp.int32, (heads, 128), 1)
        x = jnp.zeros((heads, 128), jnp.float32)
        for j, (high, total) in enumerate(pairs):
            x = jnp.where(lane == j, high, x)
            x = jnp.where(lane == STATS + j, total, x)
        mine[g, :, :heads] = x.T[: 2 * STATS, :]
        for n in range(3):
            stats(g, n).start()

    def shares(g):
        remote(theirs.at[g], theirs.at[g], stats_out, stats_in.at[g], core).wait_recv()
        rows = [mine[g]] + [theirs[g, n] for n in range(3)]
        highs, totals = [r[:STATS] for r in rows], [r[STATS:] for r in rows]
        top = jnp.maximum(jnp.maximum(highs[0], highs[1]), jnp.maximum(highs[2], highs[3]))
        scale = [jnp.exp2((h - top) * factor) for h in highs]
        parts = [t * s for t, s in zip(totals, scale)]
        whole = (parts[0] + parts[1]) + (parts[2] + parts[3])
        return (scale[0] / whole).T

    def sum_parts(what):
        kind, i = what.rstrip("0123456789"), int("0" + what.lstrip("abcdefghijklmnopqrstuvwxyz"))
        if kind == "core":
            halves(i).wait_recv()
            pair[span(i)] = add(own[span(i), rows], from_core[span(i)]).astype(jnp.bfloat16)
            sums(i).start()
        elif kind == "chip":
            sums(i).wait_recv()
            o_ref[span(i), rows] = add(pair[span(i)], from_chip[span(i)]).astype(jnp.bfloat16)
            results(i).start()
        elif kind == "late":
            to_chip(i).wait_recv()
            late_pair[i] = add(part[LATE[i]], late_chip[i]).astype(jnp.bfloat16)
            to_core(i).start()
        else:
            remote(final_in, final_in, late_out, final_sem, core).wait_recv()
            o_ref[FINAL] = (add(part[FINAL], final_in[0]) + add(final_in[1], final_in[2])).astype(jnp.bfloat16)

    pltpu.make_async_copy(q_hbm, q_ref, q_sem).start()
    reads = list(range(len(BLOCKS)))

    def start_reads(used):
        while reads and first[reads[0]] + BLOCKS[reads[0]][2] <= SLOTS + used:
            read(reads.pop(0)).start(priority=1)

    start_reads(0)
    barrier = pltpu.get_barrier_semaphore()
    for peer in peers:
        pl.semaphore_signal(barrier, inc=1, device_id=(dp, peer), device_id_type=MESH)
    pltpu.make_async_copy(q_hbm, q_ref, q_sem).wait()

    waiting, pairs, group, share = [], [], 0, {}
    for b, (kind, lo, n) in enumerate(BLOCKS):
        read(b).wait()
        if kind == "v" and lo % STATS == 0:
            share = shares(lo // STATS)
        for s in range(lo, lo + n):
            if kind == "k":
                score(s)
            else:
                gather(s, share)
            if waiting:
                pairs.append(softmax(waiting.pop(0)))
            if kind == "k":
                waiting.append(s)
        if len(pairs) >= STATS:
            if group == 0:
                pl.semaphore_wait(barrier, 3)
            send_stats(group, pairs[:STATS])
            pairs, group = pairs[STATS:], group + 1
        if kind == "v":
            if (lo, n) in SPANS:
                halves(SPANS.index((lo, n))).start()
            elif lo in LATE:
                to_chip(LATE.index(lo)).start()
        for what in SUMS.get(b, ()):
            sum_parts(what)
        if kind == "v" and lo == FINAL:
            for i in (1, 2, 0):
                to_all(i).start()
        start_reads(first[b] + n)

    for what in DRAIN:
        sum_parts(what)
    for i, s in enumerate(LATE):
        to_core(i).wait_recv()
        o_ref[s] = add(late_pair[i], late_core[i]).astype(jnp.bfloat16)

    summed = from_core.at[pl.ds(0, LATE[0])]
    remote(summed, summed, done_out, done_in, core).wait()
    remote(summed, summed, core_out, done_in, core).wait_send()
    remote(summed, summed, chip_out, done_in, core).wait_send()
    remote(theirs, theirs, stats_out, done_in, core).wait_send()
    sent = part.at[pl.ds(0, 2 * len(LATE) + 3)]
    remote(sent, sent, late_out, done_in, core).wait_send()


def solution(mesh):
    def step(q, k, v):
        count, heads, head = q.shape
        tokens = k.shape[1]
        whole = (count, heads, head)
        dma = pltpu.SemaphoreType.DMA
        hbm = pl.BlockSpec(memory_space=pltpu.HBM)
        return pl.pallas_call(
            attend,
            out_shape=jax.ShapeDtypeStruct(whole, jnp.bfloat16),
            in_specs=[hbm] * 3,
            out_specs=pl.BlockSpec(memory_space=pltpu.VMEM),
            scratch_shapes=[
                pltpu.VMEM(whole, jnp.bfloat16),
                pltpu.VMEM((SLOTS, tokens, head), jnp.bfloat16),
                pltpu.VMEM((SCORES, heads, tokens), jnp.float32),
                pltpu.VMEM((count, heads, tokens), jnp.bfloat16),
                pltpu.VMEM((count // STATS, 2 * STATS, 128), jnp.float32),
                pltpu.VMEM((count // STATS, 3, 2 * STATS, 128), jnp.float32),
                pltpu.VMEM(whole, jnp.float32),
                pltpu.VMEM(whole, jnp.bfloat16),
                *[pltpu.VMEM((count, heads // 2, head), jnp.bfloat16)] * 3,
                *[pltpu.VMEM((len(LATE), heads, head), jnp.bfloat16)] * 3,
                pltpu.VMEM((3, heads, head), jnp.bfloat16),
                dma,
                dma((READS,)),
                dma,
                dma((count // STATS,)),
                dma,
                dma((len(SPANS),)),
                dma,
                dma((len(SPANS),)),
                dma,
                dma,
                dma,
                dma((len(LATE),)),
                dma((len(LATE),)),
                dma,
            ],
            compiler_params=pltpu.CompilerParams(collective_id=0, has_side_effects=True, vmem_limit_bytes=48 * 2**20),
            name="attend",
        )(pltpu.with_memory_space_constraint(q, pltpu.HBM), k.reshape(count, tokens, head), v.reshape(count, tokens, head))

    return jax.shard_map(
        step,
        mesh=mesh,
        in_specs=(P("dp", None, None), P("dp", "sp", None, None), P("dp", "sp", None, None)),
        out_specs=P("dp", None, None),
        check_vma=False,
    )
```

```python
import jax
import jax.numpy as jnp
from jax import lax
from jax.experimental import pallas as pl
from jax.experimental.pallas import tpu as pltpu
from jax.sharding import PartitionSpec as P

MESH = pl.DeviceIdType.MESH
LOG2E = 1.4426950408889634
SLOTS = 32
READS = 8
BYROWS = 24
STATS = 8
SCORES = 4

BLOCKS = (
    ("k", 0, 4),
    ("k", 4, 4),
    ("k", 8, 4),
    ("k", 12, 4),
    ("k", 16, 4),
    ("k", 20, 4),
    ("k", 24, 4),
    ("k", 28, 4),
    ("v", 0, 4),
    ("v", 4, 4),
    ("v", 8, 4),
    ("v", 12, 4),
    ("v", 16, 2),
    ("v", 18, 2),
    ("v", 20, 2),
    ("v", 22, 2),
    ("v", 24, 1),
    ("v", 25, 1),
    ("v", 26, 1),
    ("v", 27, 1),
    ("v", 28, 1),
    ("v", 29, 1),
    ("v", 30, 1),
    ("v", 31, 1),
)
LATE = (29, 30)
FINAL = (31,)
SPANS = ((0, 8), (8, 8), (16, 4), (20, 4), (24, 1), (25, 1), (26, 1), (27, 1), (28, 1))
SUMS = {
    10: ("core0",),
    13: ("core1",),
    15: ("core2",),
    16: ("chip0",),
    18: ("core3",),
    19: ("core4",),
    20: ("core5",),
    21: ("core6",),
    22: ("core7",),
    23: ("core8", "chip1"),
}
DRAIN = ("chip2", "chip3", "chip4", "chip5", "chip6", "late0", "chip7", "late1", "chip8", "final0")

def attend(q_hbm, k_hbm, v_hbm, o_ref, q_ref, buf, scores, weights, mine, theirs, own, part, from_core, pair, from_chip, late_pair, late_chip, late_core, final_in,
           q_sem, buf_sem, stats_out, stats_in, core_out, core_in, chip_out, chip_in, done_out, done_in, late_out, late_chip_in, late_core_in, final_sem):
    count, heads, head = q_hbm.shape
    half = heads // 2
    factor = head**-0.5 * LOG2E

    dp, sp = lax.axis_index("dp"), lax.axis_index("sp")
    side = lax.rem(sp, 2)
    core = sp + 1 - 2 * side
    chip = lax.rem(sp + 2, 4)
    peers = (core, chip, lax.rem(core + 2, 4))
    rows = pl.ds(pl.multiple_of(side * half, half), half)
    other_rows = pl.ds(pl.multiple_of((1 - side) * half, half), half)

    first = [sum(n for _, _, n in BLOCKS[:b]) for b in range(len(BLOCKS))]
    slot_of = {(kind, s + i): (first[b] + i) % SLOTS for b, (kind, s, n) in enumerate(BLOCKS) for i in range(n)}

    def read(b):
        kind, s, n = BLOCKS[b]
        src = k_hbm if kind == "k" else v_hbm
        return pltpu.make_async_copy(src.at[pl.ds(s, n)], buf.at[pl.ds(first[b] % SLOTS, n)], buf_sem.at[b % READS])

    def remote(src, dst, send, recv, peer):
        return pltpu.make_async_remote_copy(src, dst, send, recv, device_id=(dp, peer), device_id_type=MESH)

    def stats(g, n):
        return remote(mine.at[g], theirs.at[g, n], stats_out, stats_in.at[g], peers[n])

    def span(c):
        return pl.ds(*SPANS[c])

    def halves(c):
        return remote(part.at[span(c), other_rows], from_core.at[span(c)], core_out, core_in.at[c], core)

    def sums(c):
        return remote(pair.at[span(c)], from_chip.at[span(c)], chip_out, chip_in.at[c], chip)

    def results(c):
        return remote(o_ref.at[span(c), rows], o_ref.at[span(c), rows], done_out, done_in, core)

    def to_chip(i):
        return remote(part.at[LATE[i]], late_chip.at[i], late_out, late_chip_in.at[i], chip)

    def to_core(i):
        return remote(late_pair.at[i], late_core.at[i], late_out, late_core_in.at[i], core)

    def to_all(i, n):
        return remote(part.at[FINAL[i]], final_in.at[i, n], late_out, final_sem.at[i], peers[n])

    def add(a, b):
        return a.astype(jnp.float32) + b.astype(jnp.float32)

    def score(s):
        scores[s % SCORES] = lax.dot_general(
            q_ref[s], buf[slot_of["k", s]], (((1,), (1,)), ((), ())), preferred_element_type=jnp.float32
        )

    def softmax(s):
        x = scores[s % SCORES]
        high = jnp.max(x, 1, keepdims=True)
        w = jnp.exp2((x - high) * factor)
        weights[s] = w.astype(jnp.bfloat16)
        return high, jnp.sum(w, 1, keepdims=True)

    def gather(s, share):
        v = slot_of["v", s]
        share = share[:heads, s % STATS : s % STATS + 1]
        if s < BYROWS:
            seen = [jnp.dot(weights[s], buf[v, :, c : c + 128], preferred_element_type=jnp.float32) for c in range(0, head, 128)]
            seen = jnp.concatenate(seen, 1) * share
        else:
            cut = buf.shape[1] // 2
            seen = [jnp.dot(weights[s, :, c : c + cut], buf[v, c : c + cut], preferred_element_type=jnp.float32) * share for c in (0, cut)]
            seen = seen[0] + seen[1]
        own[s] = seen
        part[s] = seen.astype(jnp.bfloat16)

    def send_stats(g, pairs):
        lane = lax.broadcasted_iota(jnp.int32, (heads, 128), 1)
        x = jnp.zeros((heads, 128), jnp.float32)
        for j, (high, total) in enumerate(pairs):
            x = jnp.where(lane == j, high, x)
            x = jnp.where(lane == STATS + j, total, x)
        mine[g, :, :heads] = x.T[: 2 * STATS, :]
        for n in range(3):
            stats(g, n).start()

    def shares(g):
        remote(theirs.at[g], theirs.at[g], stats_out, stats_in.at[g], core).wait_recv()
        rows = [mine[g]] + [theirs[g, n] for n in range(3)]
        highs, totals = [r[:STATS] for r in rows], [r[STATS:] for r in rows]
        top = jnp.maximum(jnp.maximum(highs[0], highs[1]), jnp.maximum(highs[2], highs[3]))
        scale = [jnp.exp2((h - top) * factor) for h in highs]
        parts = [t * s for t, s in zip(totals, scale)]
        whole = (parts[0] + parts[1]) + (parts[2] + parts[3])
        return (scale[0] / whole).T

    def sum_parts(what):
        kind, i = what.rstrip("0123456789"), int("0" + what.lstrip("abcdefghijklmnopqrstuvwxyz"))
        if kind == "core":
            halves(i).wait_recv()
            pair[span(i)] = add(own[span(i), rows], from_core[span(i)]).astype(jnp.bfloat16)
            sums(i).start()
        elif kind == "chip":
            sums(i).wait_recv()
            o_ref[span(i), rows] = add(pair[span(i)], from_chip[span(i)]).astype(jnp.bfloat16)
            results(i).start()
        elif kind == "late":
            to_chip(i).wait_recv()
            late_pair[i] = add(part[LATE[i]], late_chip[i]).astype(jnp.bfloat16)
            to_core(i).start()
        else:
            remote(final_in.at[i], final_in.at[i], late_out, final_sem.at[i], core).wait_recv()
            o_ref[FINAL[i]] = (add(part[FINAL[i]], final_in[i, 0]) + add(final_in[i, 1], final_in[i, 2])).astype(jnp.bfloat16)

    pltpu.make_async_copy(q_hbm, q_ref, q_sem).start()
    reads = list(range(len(BLOCKS)))

    def start_reads(done, used):
        while reads and reads[0] < READS + done and first[reads[0]] + BLOCKS[reads[0]][2] <= SLOTS + used:
            read(reads.pop(0)).start(priority=1)

    start_reads(0, 0)
    barrier = pltpu.get_barrier_semaphore()
    for peer in peers:
        pl.semaphore_signal(barrier, inc=1, device_id=(dp, peer), device_id_type=MESH)
    pltpu.make_async_copy(q_hbm, q_ref, q_sem).wait()

    waiting, pairs, group, share = [], [], 0, {}
    for b, (kind, lo, n) in enumerate(BLOCKS):
        read(b).wait()
        if kind == "v" and lo % STATS == 0:
            share = shares(lo // STATS)
        for s in range(lo, lo + n):
            if kind == "k":
                score(s)
            else:
                gather(s, share)
            if waiting:
                pairs.append(softmax(waiting.pop(0)))
            if kind == "k":
                waiting.append(s)
        if len(pairs) >= STATS:
            if group == 0:
                pl.semaphore_wait(barrier, 3)
            send_stats(group, pairs[:STATS])
            pairs, group = pairs[STATS:], group + 1
        if kind == "v":
            for c, (s, m) in enumerate(SPANS):
                if s + m == lo + n:
                    halves(c).start()
            if lo in LATE:
                to_chip(LATE.index(lo)).start()
        for what in SUMS.get(b, ()):
            sum_parts(what)
        if kind == "v" and lo in FINAL:
            for peer in (1, 2, 0):
                to_all(FINAL.index(lo), peer).start()
        start_reads(b + 1, first[b] + n)

    for what in DRAIN:
        sum_parts(what)
    for i, s in enumerate(LATE):
        to_core(i).wait_recv()
        o_ref[s] = add(late_pair[i], late_core[i]).astype(jnp.bfloat16)

    summed = from_core.at[pl.ds(0, sum(n for _, n in SPANS))]
    remote(summed, summed, done_out, done_in, core).wait()
    remote(summed, summed, core_out, done_in, core).wait_send()
    remote(summed, summed, chip_out, done_in, core).wait_send()
    remote(theirs, theirs, stats_out, done_in, core).wait_send()
    sent = part.at[pl.ds(0, 2 * len(LATE) + 3 * len(FINAL))]
    remote(sent, sent, late_out, done_in, core).wait_send()


def solution(mesh):
    def step(q, k, v):
        count, heads, head = q.shape
        tokens = k.shape[1]
        whole = (count, heads, head)
        dma = pltpu.SemaphoreType.DMA
        hbm = pl.BlockSpec(memory_space=pltpu.HBM)
        return pl.pallas_call(
            attend,
            out_shape=jax.ShapeDtypeStruct(whole, jnp.bfloat16),
            in_specs=[hbm] * 3,
            out_specs=pl.BlockSpec(memory_space=pltpu.VMEM),
            scratch_shapes=[
                pltpu.VMEM(whole, jnp.bfloat16),
                pltpu.VMEM((SLOTS, tokens, head), jnp.bfloat16),
                pltpu.VMEM((SCORES, heads, tokens), jnp.float32),
                pltpu.VMEM((count, heads, tokens), jnp.bfloat16),
                pltpu.VMEM((count // STATS, 2 * STATS, 128), jnp.float32),
                pltpu.VMEM((count // STATS, 3, 2 * STATS, 128), jnp.float32),
                pltpu.VMEM(whole, jnp.float32),
                pltpu.VMEM(whole, jnp.bfloat16),
                *[pltpu.VMEM((count, heads // 2, head), jnp.bfloat16)] * 3,
                *[pltpu.VMEM((len(LATE), heads, head), jnp.bfloat16)] * 3,
                pltpu.VMEM((len(FINAL), 3, heads, head), jnp.bfloat16),
                dma,
                dma((READS,)),
                dma,
                dma((count // STATS,)),
                dma,
                dma((len(SPANS),)),
                dma,
                dma((len(SPANS),)),
                dma,
                dma,
                dma,
                dma((len(LATE),)),
                dma((len(LATE),)),
                dma((len(FINAL),)),
            ],
            compiler_params=pltpu.CompilerParams(collective_id=0, has_side_effects=True, vmem_limit_bytes=48 * 2**20),
            name="attend",
        )(pltpu.with_memory_space_constraint(q, pltpu.HBM), k.reshape(count, tokens, head), v.reshape(count, tokens, head))

    return jax.shard_map(
        step,
        mesh=mesh,
        in_specs=(P("dp", None, None), P("dp", "sp", None, None), P("dp", "sp", None, None)),
        out_specs=P("dp", None, None),
        check_vma=False,
    )
```

```python
import jax
import jax.numpy as jnp
from jax import lax
from jax.experimental import pallas as pl
from jax.experimental.pallas import tpu as pltpu
from jax.sharding import PartitionSpec as P

MESH = pl.DeviceIdType.MESH
LOG2E = 1.4426950408889634
SLOTS = 32
READS = 6
BYROWS = 24
STATS = 16
SCORES = 4

BLOCKS = (
    ("k", 0, 4),
    ("k", 4, 4),
    ("k", 8, 4),
    ("k", 12, 4),
    ("k", 16, 4),
    ("k", 20, 4),
    ("k", 24, 4),
    ("k", 28, 4),
    ("v", 0, 4),
    ("v", 4, 4),
    ("v", 8, 4),
    ("v", 12, 4),
    ("v", 16, 2),
    ("v", 18, 2),
    ("v", 20, 2),
    ("v", 22, 2),
    ("v", 24, 1),
    ("v", 25, 1),
    ("v", 26, 1),
    ("v", 27, 1),
    ("v", 28, 1),
    ("v", 29, 1),
    ("v", 30, 1),
    ("v", 31, 1),
)
LATE = (29, 30)
FINAL = (31,)
SPANS = ((0, 8), (8, 8), (16, 4), (20, 4), (24, 1), (25, 1), (26, 1), (27, 2))
SUMS = {
    10: ("core0",),
    13: ("core1",),
    15: ("core2",),
    16: ("chip0",),
    18: ("core3",),
    19: ("core4",),
    20: ("core5",),
    21: ("core6",),
    23: ("core7", "chip1"),
}
DRAIN = ("chip2", "chip3", "chip4", "chip5", "chip6", "late0", "late1", "chip7", "final0")

def attend(q_hbm, k_hbm, v_hbm, o_ref, q_ref, buf, scores, weights, mine, theirs, own, part, from_core, pair, from_chip, late_pair, late_chip, late_core, final_in,
           q_sem, buf_sem, stats_out, stats_in, core_out, core_in, chip_out, chip_in, done_out, done_in, late_out, late_chip_in, late_core_in, final_sem):
    count, heads, head = q_hbm.shape
    half = heads // 2
    factor = head**-0.5 * LOG2E

    dp, sp = lax.axis_index("dp"), lax.axis_index("sp")
    side = lax.rem(sp, 2)
    core = sp + 1 - 2 * side
    chip = lax.rem(sp + 2, 4)
    peers = (core, chip, lax.rem(core + 2, 4))
    rows = pl.ds(pl.multiple_of(side * half, half), half)
    other_rows = pl.ds(pl.multiple_of((1 - side) * half, half), half)

    first = [sum(n for _, _, n in BLOCKS[:b]) for b in range(len(BLOCKS))]
    slot_of = {(kind, s + i): (first[b] + i) % SLOTS for b, (kind, s, n) in enumerate(BLOCKS) for i in range(n)}

    def read(b):
        kind, s, n = BLOCKS[b]
        src = k_hbm if kind == "k" else v_hbm
        return pltpu.make_async_copy(src.at[pl.ds(s, n)], buf.at[pl.ds(first[b] % SLOTS, n)], buf_sem.at[b % READS])

    def remote(src, dst, send, recv, peer):
        return pltpu.make_async_remote_copy(src, dst, send, recv, device_id=(dp, peer), device_id_type=MESH)

    def stats(g, n):
        return remote(mine.at[g], theirs.at[g, n], stats_out, stats_in.at[g], peers[n])

    def span(c):
        return pl.ds(*SPANS[c])

    def halves(c):
        return remote(part.at[span(c), other_rows], from_core.at[span(c)], core_out, core_in.at[c], core)

    def sums(c):
        return remote(pair.at[span(c)], from_chip.at[span(c)], chip_out, chip_in.at[c], chip)

    def results(c):
        return remote(o_ref.at[span(c), rows], o_ref.at[span(c), rows], done_out, done_in, core)

    def to_chip(i):
        return remote(part.at[LATE[i]], late_chip.at[i], late_out, late_chip_in.at[i], chip)

    def to_core(i):
        return remote(late_pair.at[i], late_core.at[i], late_out, late_core_in.at[i], core)

    def to_all(i, n):
        return remote(part.at[FINAL[i]], final_in.at[i, n], late_out, final_sem.at[i], peers[n])

    def add(a, b):
        return a.astype(jnp.float32) + b.astype(jnp.float32)

    def score(s):
        scores[s % SCORES] = lax.dot_general(
            q_ref[s], buf[slot_of["k", s]], (((1,), (1,)), ((), ())), preferred_element_type=jnp.float32
        )

    def softmax(s):
        x = scores[s % SCORES]
        high = jnp.max(x, 1, keepdims=True)
        w = jnp.exp2((x - high) * factor)
        weights[s] = w.astype(jnp.bfloat16)
        return high, jnp.sum(w, 1, keepdims=True)

    def gather(s, share):
        v = slot_of["v", s]
        share = share[:heads, s % STATS : s % STATS + 1]
        if s < BYROWS:
            seen = [jnp.dot(weights[s], buf[v, :, c : c + 128], preferred_element_type=jnp.float32) for c in range(0, head, 128)]
            seen = jnp.concatenate(seen, 1) * share
        else:
            cut = buf.shape[1] // 2
            seen = [jnp.dot(weights[s, :, c : c + cut], buf[v, c : c + cut], preferred_element_type=jnp.float32) * share for c in (0, cut)]
            seen = seen[0] + seen[1]
        own[s] = seen
        part[s] = seen.astype(jnp.bfloat16)

    def send_stats(g, pairs):
        lane = lax.broadcasted_iota(jnp.int32, (heads, 128), 1)
        x = jnp.zeros((heads, 128), jnp.float32)
        for j, (high, total) in enumerate(pairs):
            x = jnp.where(lane == j, high, x)
            x = jnp.where(lane == STATS + j, total, x)
        mine[g, :, :heads] = x.T[: 2 * STATS, :]
        for n in range(3):
            stats(g, n).start()

    def shares(g):
        remote(theirs.at[g], theirs.at[g], stats_out, stats_in.at[g], core).wait_recv()
        rows = [mine[g]] + [theirs[g, n] for n in range(3)]
        highs, totals = [r[:STATS] for r in rows], [r[STATS:] for r in rows]
        top = jnp.maximum(jnp.maximum(highs[0], highs[1]), jnp.maximum(highs[2], highs[3]))
        scale = [jnp.exp2((h - top) * factor) for h in highs]
        parts = [t * s for t, s in zip(totals, scale)]
        whole = (parts[0] + parts[1]) + (parts[2] + parts[3])
        return (scale[0] / whole).T

    def sum_parts(what):
        kind, i = what.rstrip("0123456789"), int("0" + what.lstrip("abcdefghijklmnopqrstuvwxyz"))
        if kind == "core":
            halves(i).wait_recv()
            pair[span(i)] = add(own[span(i), rows], from_core[span(i)]).astype(jnp.bfloat16)
            sums(i).start()
        elif kind == "chip":
            sums(i).wait_recv()
            o_ref[span(i), rows] = add(pair[span(i)], from_chip[span(i)]).astype(jnp.bfloat16)
            results(i).start()
        elif kind == "late":
            to_chip(i).wait_recv()
            late_pair[i] = add(part[LATE[i]], late_chip[i]).astype(jnp.bfloat16)
            to_core(i).start()
        else:
            remote(final_in.at[i], final_in.at[i], late_out, final_sem.at[i], core).wait_recv()
            o_ref[FINAL[i]] = (add(part[FINAL[i]], final_in[i, 0]) + add(final_in[i, 1], final_in[i, 2])).astype(jnp.bfloat16)

    pltpu.make_async_copy(q_hbm, q_ref, q_sem).start()
    reads = list(range(len(BLOCKS)))

    def start_reads(done, used):
        while reads and reads[0] < READS + done and first[reads[0]] + BLOCKS[reads[0]][2] <= SLOTS + used:
            read(reads.pop(0)).start(priority=1)

    start_reads(0, 0)
    barrier = pltpu.get_barrier_semaphore()
    for peer in peers:
        pl.semaphore_signal(barrier, inc=1, device_id=(dp, peer), device_id_type=MESH)
    pltpu.make_async_copy(q_hbm, q_ref, q_sem).wait()

    waiting, pairs, group, share = [], [], 0, {}
    for b, (kind, lo, n) in enumerate(BLOCKS):
        read(b).wait()
        if kind == "v" and lo % STATS == 0:
            share = shares(lo // STATS)
        for s in range(lo, lo + n):
            if kind == "k":
                score(s)
            else:
                gather(s, share)
            if waiting:
                pairs.append(softmax(waiting.pop(0)))
            if kind == "k":
                waiting.append(s)
        if len(pairs) >= STATS:
            if group == 0:
                pl.semaphore_wait(barrier, 3)
            send_stats(group, pairs[:STATS])
            pairs, group = pairs[STATS:], group + 1
        if kind == "v":
            for c, (s, m) in enumerate(SPANS):
                if s + m == lo + n:
                    halves(c).start()
            if lo in LATE:
                to_chip(LATE.index(lo)).start()
        for what in SUMS.get(b, ()):
            sum_parts(what)
        if kind == "v" and lo in FINAL:
            for peer in (1, 2, 0):
                to_all(FINAL.index(lo), peer).start()
        start_reads(b + 1, first[b] + n)

    for what in DRAIN:
        sum_parts(what)
    for i, s in enumerate(LATE):
        to_core(i).wait_recv()
        o_ref[s] = add(late_pair[i], late_core[i]).astype(jnp.bfloat16)

    summed = from_core.at[pl.ds(0, sum(n for _, n in SPANS))]
    remote(summed, summed, done_out, done_in, core).wait()
    remote(summed, summed, core_out, done_in, core).wait_send()
    remote(summed, summed, chip_out, done_in, core).wait_send()
    remote(theirs, theirs, stats_out, done_in, core).wait_send()
    sent = part.at[pl.ds(0, 2 * len(LATE) + 3 * len(FINAL))]
    remote(sent, sent, late_out, done_in, core).wait_send()


def solution(mesh):
    def step(q, k, v):
        count, heads, head = q.shape
        tokens = k.shape[1]
        whole = (count, heads, head)
        dma = pltpu.SemaphoreType.DMA
        hbm = pl.BlockSpec(memory_space=pltpu.HBM)
        return pl.pallas_call(
            attend,
            out_shape=jax.ShapeDtypeStruct(whole, jnp.bfloat16),
            in_specs=[hbm] * 3,
            out_specs=pl.BlockSpec(memory_space=pltpu.VMEM),
            scratch_shapes=[
                pltpu.VMEM(whole, jnp.bfloat16),
                pltpu.VMEM((SLOTS, tokens, head), jnp.bfloat16),
                pltpu.VMEM((SCORES, heads, tokens), jnp.float32),
                pltpu.VMEM((count, heads, tokens), jnp.bfloat16),
                pltpu.VMEM((count // STATS, 2 * STATS, 128), jnp.float32),
                pltpu.VMEM((count // STATS, 3, 2 * STATS, 128), jnp.float32),
                pltpu.VMEM(whole, jnp.float32),
                pltpu.VMEM(whole, jnp.bfloat16),
                *[pltpu.VMEM((count, heads // 2, head), jnp.bfloat16)] * 3,
                *[pltpu.VMEM((len(LATE), heads, head), jnp.bfloat16)] * 3,
                pltpu.VMEM((len(FINAL), 3, heads, head), jnp.bfloat16),
                dma,
                dma((READS,)),
                dma,
                dma((count // STATS,)),
                dma,
                dma((len(SPANS),)),
                dma,
                dma((len(SPANS),)),
                dma,
                dma,
                dma,
                dma((len(LATE),)),
                dma((len(LATE),)),
                dma((len(FINAL),)),
            ],
            compiler_params=pltpu.CompilerParams(collective_id=0, has_side_effects=True, vmem_limit_bytes=48 * 2**20),
            name="attend",
        )(pltpu.with_memory_space_constraint(q, pltpu.HBM), k.reshape(count, tokens, head), v.reshape(count, tokens, head))

    return jax.shard_map(
        step,
        mesh=mesh,
        in_specs=(P("dp", None, None), P("dp", "sp", None, None), P("dp", "sp", None, None)),
        out_specs=P("dp", None, None),
        check_vma=False,
    )
```

```python
import jax
import jax.numpy as jnp
from jax import lax
from jax.experimental import pallas as pl
from jax.experimental.pallas import tpu as pltpu
from jax.sharding import PartitionSpec as P

MESH = pl.DeviceIdType.MESH
LOG2E = 1.4426950408889634
SLOTS = 32
READS = 6
BYROWS = 24
STATS = 16
SCORES = 4

BLOCKS = (
    ("k", 0, 4),
    ("k", 4, 4),
    ("k", 8, 4),
    ("k", 12, 4),
    ("k", 16, 4),
    ("k", 20, 4),
    ("k", 24, 4),
    ("k", 28, 4),
    ("v", 0, 4),
    ("v", 4, 4),
    ("v", 8, 4),
    ("v", 12, 4),
    ("v", 16, 2),
    ("v", 18, 2),
    ("v", 20, 2),
    ("v", 22, 2),
    ("v", 24, 1),
    ("v", 25, 1),
    ("v", 26, 1),
    ("v", 27, 1),
    ("v", 28, 1),
    ("v", 29, 1),
    ("v", 30, 1),
    ("v", 31, 1),
)
LATE = (29, 30)
FINAL = (31,)
SPANS = ((0, 8), (8, 8), (16, 4), (20, 4), (24, 1), (25, 1), (26, 1), (27, 2))
CHIP_SEM = (0, 1, 2, 2, 3, 3, 4, 5)
SUMS = {
    10: ("core0",),
    13: ("core1",),
    15: ("core2",),
    16: ("chip0",),
    18: ("core3",),
    19: ("core4",),
    20: ("core5",),
    21: ("core6",),
    23: ("core7", "chip1"),
}
DRAIN = ("chip2", "chip3", "chip4", "chip5", "chip6", "late0", "late1", "chip7", "final0")

def attend(q_hbm, k_hbm, v_hbm, o_ref, q_ref, buf, scores, weights, mine, theirs, own, part, from_core, pair, from_chip, late_pair, late_chip, late_core, final_in,
           q_sem, buf_sem, stats_out, stats_in, core_out, core_in, chip_out, chip_in, done_out, done_in, late_out, late_chip_in, late_core_in, final_sem):
    count, heads, head = q_hbm.shape
    half = heads // 2
    factor = head**-0.5 * LOG2E

    dp, sp = lax.axis_index("dp"), lax.axis_index("sp")
    side = lax.rem(sp, 2)
    core = sp + 1 - 2 * side
    chip = lax.rem(sp + 2, 4)
    peers = (core, chip, lax.rem(core + 2, 4))
    rows = pl.ds(pl.multiple_of(side * half, half), half)
    other_rows = pl.ds(pl.multiple_of((1 - side) * half, half), half)

    first = [sum(n for _, _, n in BLOCKS[:b]) for b in range(len(BLOCKS))]
    slot_of = {(kind, s + i): (first[b] + i) % SLOTS for b, (kind, s, n) in enumerate(BLOCKS) for i in range(n)}

    def read(b):
        kind, s, n = BLOCKS[b]
        src = k_hbm if kind == "k" else v_hbm
        return pltpu.make_async_copy(src.at[pl.ds(s, n)], buf.at[pl.ds(first[b] % SLOTS, n)], buf_sem.at[b % READS])

    def remote(src, dst, send, recv, peer):
        return pltpu.make_async_remote_copy(src, dst, send, recv, device_id=(dp, peer), device_id_type=MESH)

    def stats(g, n):
        return remote(mine.at[g], theirs.at[g, n], stats_out, stats_in.at[g], peers[n])

    def span(c):
        return pl.ds(*SPANS[c])

    def halves(c):
        return remote(part.at[span(c), other_rows], from_core.at[span(c)], core_out, core_in.at[c], core)

    def sums(c):
        return remote(pair.at[span(c)], from_chip.at[span(c)], chip_out, chip_in.at[CHIP_SEM[c]], chip)

    def results(c):
        return remote(o_ref.at[span(c), rows], o_ref.at[span(c), rows], done_out, done_in, core)

    def to_chip(i):
        return remote(part.at[LATE[i]], late_chip.at[i], late_out, late_chip_in.at[i], chip)

    def to_core(i):
        return remote(late_pair.at[i], late_core.at[i], late_out, late_core_in, core)

    def to_all(i, n):
        return remote(part.at[FINAL[i]], final_in.at[i, n], late_out, final_sem.at[i], peers[n])

    def add(a, b):
        return a.astype(jnp.float32) + b.astype(jnp.float32)

    def score(s):
        scores[s % SCORES] = lax.dot_general(
            q_ref[s], buf[slot_of["k", s]], (((1,), (1,)), ((), ())), preferred_element_type=jnp.float32
        )

    def softmax(s):
        x = scores[s % SCORES]
        high = jnp.max(x, 1, keepdims=True)
        w = jnp.exp2((x - high) * factor)
        weights[s] = w.astype(jnp.bfloat16)
        return high, jnp.sum(w, 1, keepdims=True)

    def gather(s, share):
        v = slot_of["v", s]
        share = share[:heads, s % STATS : s % STATS + 1]
        if s < BYROWS:
            seen = [jnp.dot(weights[s], buf[v, :, c : c + 128], preferred_element_type=jnp.float32) for c in range(0, head, 128)]
            seen = jnp.concatenate(seen, 1) * share
        else:
            cut = buf.shape[1] // 2
            seen = [jnp.dot(weights[s, :, c : c + cut], buf[v, c : c + cut], preferred_element_type=jnp.float32) * share for c in (0, cut)]
            seen = seen[0] + seen[1]
        own[s] = seen
        part[s] = seen.astype(jnp.bfloat16)

    def send_stats(g, pairs):
        lane = lax.broadcasted_iota(jnp.int32, (heads, 128), 1)
        x = jnp.zeros((heads, 128), jnp.float32)
        for j, (high, total) in enumerate(pairs):
            x = jnp.where(lane == j, high, x)
            x = jnp.where(lane == STATS + j, total, x)
        mine[g, :, :heads] = x.T[: 2 * STATS, :]
        for n in range(3):
            stats(g, n).start()

    def shares(g):
        remote(theirs.at[g], theirs.at[g], stats_out, stats_in.at[g], core).wait_recv()
        rows = [mine[g]] + [theirs[g, n] for n in range(3)]
        highs, totals = [r[:STATS] for r in rows], [r[STATS:] for r in rows]
        top = jnp.maximum(jnp.maximum(highs[0], highs[1]), jnp.maximum(highs[2], highs[3]))
        scale = [jnp.exp2((h - top) * factor) for h in highs]
        parts = [t * s for t, s in zip(totals, scale)]
        whole = (parts[0] + parts[1]) + (parts[2] + parts[3])
        return (scale[0] / whole).T

    def sum_parts(what):
        kind, i = what.rstrip("0123456789"), int("0" + what.lstrip("abcdefghijklmnopqrstuvwxyz"))
        if kind == "core":
            halves(i).wait_recv()
            pair[span(i)] = add(own[span(i), rows], from_core[span(i)]).astype(jnp.bfloat16)
            sums(i).start()
        elif kind == "chip":
            if i == 0 or CHIP_SEM[i] != CHIP_SEM[i - 1]:
                joint = [SPANS[c] for c in range(len(SPANS)) if CHIP_SEM[c] == CHIP_SEM[i]]
                arrived = from_chip.at[pl.ds(SPANS[i][0], sum(n for _, n in joint))]
                remote(arrived, arrived, chip_out, chip_in.at[CHIP_SEM[i]], chip).wait_recv()
            o_ref[span(i), rows] = add(pair[span(i)], from_chip[span(i)]).astype(jnp.bfloat16)
            results(i).start()
        elif kind == "late":
            to_chip(i).wait_recv()
            late_pair[i] = add(part[LATE[i]], late_chip[i]).astype(jnp.bfloat16)
            to_core(i).start()
        else:
            remote(final_in.at[i], final_in.at[i], late_out, final_sem.at[i], core).wait_recv()
            o_ref[FINAL[i]] = (add(part[FINAL[i]], final_in[i, 0]) + add(final_in[i, 1], final_in[i, 2])).astype(jnp.bfloat16)

    pltpu.make_async_copy(q_hbm, q_ref, q_sem).start()
    reads = list(range(len(BLOCKS)))

    def start_reads(done, used):
        while reads and reads[0] < READS + done and first[reads[0]] + BLOCKS[reads[0]][2] <= SLOTS + used:
            read(reads.pop(0)).start(priority=1)

    start_reads(0, 0)
    barrier = pltpu.get_barrier_semaphore()
    for peer in peers:
        pl.semaphore_signal(barrier, inc=1, device_id=(dp, peer), device_id_type=MESH)
    pltpu.make_async_copy(q_hbm, q_ref, q_sem).wait()

    waiting, pairs, group, share = [], [], 0, {}
    for b, (kind, lo, n) in enumerate(BLOCKS):
        read(b).wait()
        if kind == "v" and lo % STATS == 0:
            share = shares(lo // STATS)
        for s in range(lo, lo + n):
            if kind == "k":
                score(s)
            else:
                gather(s, share)
            if waiting:
                pairs.append(softmax(waiting.pop(0)))
            if kind == "k":
                waiting.append(s)
        if len(pairs) >= STATS:
            if group == 0:
                pl.semaphore_wait(barrier, 3)
            send_stats(group, pairs[:STATS])
            pairs, group = pairs[STATS:], group + 1
        if kind == "v":
            for c, (s, m) in enumerate(SPANS):
                if s + m == lo + n:
                    halves(c).start()
            if lo in LATE:
                to_chip(LATE.index(lo)).start()
        for what in SUMS.get(b, ()):
            sum_parts(what)
        if kind == "v" and lo in FINAL:
            for peer in (1, 2, 0):
                to_all(FINAL.index(lo), peer).start()
        start_reads(b + 1, first[b] + n)

    for what in DRAIN:
        sum_parts(what)
    remote(late_core, late_core, late_out, late_core_in, core).wait_recv()
    for i, s in enumerate(LATE):
        o_ref[s] = add(late_pair[i], late_core[i]).astype(jnp.bfloat16)

    summed = from_core.at[pl.ds(0, sum(n for _, n in SPANS))]
    remote(summed, summed, done_out, done_in, core).wait()
    remote(summed, summed, core_out, done_in, core).wait_send()
    remote(summed, summed, chip_out, done_in, core).wait_send()
    remote(theirs, theirs, stats_out, done_in, core).wait_send()
    sent = part.at[pl.ds(0, 2 * len(LATE) + 3 * len(FINAL))]
    remote(sent, sent, late_out, done_in, core).wait_send()


def solution(mesh):
    def step(q, k, v):
        count, heads, head = q.shape
        tokens = k.shape[1]
        whole = (count, heads, head)
        dma = pltpu.SemaphoreType.DMA
        hbm = pl.BlockSpec(memory_space=pltpu.HBM)
        return pl.pallas_call(
            attend,
            out_shape=jax.ShapeDtypeStruct(whole, jnp.bfloat16),
            in_specs=[hbm] * 3,
            out_specs=pl.BlockSpec(memory_space=pltpu.VMEM),
            scratch_shapes=[
                pltpu.VMEM(whole, jnp.bfloat16),
                pltpu.VMEM((SLOTS, tokens, head), jnp.bfloat16),
                pltpu.VMEM((SCORES, heads, tokens), jnp.float32),
                pltpu.VMEM((count, heads, tokens), jnp.bfloat16),
                pltpu.VMEM((count // STATS, 2 * STATS, 128), jnp.float32),
                pltpu.VMEM((count // STATS, 3, 2 * STATS, 128), jnp.float32),
                pltpu.VMEM(whole, jnp.float32),
                pltpu.VMEM(whole, jnp.bfloat16),
                *[pltpu.VMEM((count, heads // 2, head), jnp.bfloat16)] * 3,
                *[pltpu.VMEM((len(LATE), heads, head), jnp.bfloat16)] * 3,
                pltpu.VMEM((len(FINAL), 3, heads, head), jnp.bfloat16),
                dma,
                dma((READS,)),
                dma,
                dma((count // STATS,)),
                dma,
                dma((len(SPANS),)),
                dma,
                dma((max(CHIP_SEM) + 1,)),
                dma,
                dma,
                dma,
                dma((len(LATE),)),
                dma,
                dma((len(FINAL),)),
            ],
            compiler_params=pltpu.CompilerParams(collective_id=0, has_side_effects=True, vmem_limit_bytes=48 * 2**20),
            name="attend",
        )(pltpu.with_memory_space_constraint(q, pltpu.HBM), k.reshape(count, tokens, head), v.reshape(count, tokens, head))

    return jax.shard_map(
        step,
        mesh=mesh,
        in_specs=(P("dp", None, None), P("dp", "sp", None, None), P("dp", "sp", None, None)),
        out_specs=P("dp", None, None),
        check_vma=False,
    )
```
